32 devices in a mesh: groups: 2 (over y), row: 4 (over z), col: 2 (over x), mp: 2 (over core).
Axes of the slice: x: 2, y: 2, z: 4, core: 2. Of those that a mesh axis runs over, the one named last changes fastest.
Arguments:
- queries: bfloat16 [2, 2048, 5120], P('mp', ('groups', 'row'), 'col'), parts along dimension 1, may hold values from -6 to 6
- keys: bfloat16 [2, 2048, 1024], P('mp', ('groups', 'row'), 'col'), parts along dimension 1, may hold values from -6 to 6
- values: bfloat16 [2, 2048, 1024], P('mp', ('groups', 'row'), 'col'), parts along dimension 1, may hold values from -6 to 6
- lengths: int32 [4], P('groups'), parts along dimension 0, may hold values from 1 to 768, 1024 in all
Outputs:
- outputs: bfloat16 [2, 2048, 5120], P('mp', ('groups', 'row'), 'col'), parts along dimension 1
- gap: float32 [40, 2048], P(('col', 'mp'), ('groups', 'row')), parts along dimension 1
The draws below stay inside these ranges and needn't reach their ends.
There are 2 independent parts, one for each index of `groups`. The reference program is written for one: setup_inputs(seed, part) draws one part's arguments, and reference() takes and returns one part's arrays. A program takes and returns all parts, laid end to end along the dimension named above; each array names one. Nothing has to cross between parts.
Inputs may be any that keep to these rules, and one draw needn't show every extreme that they name: The 2 lengths sum to 1024; one rollout is exactly 768 tokens long.
All inputs are finite; a program needn't handle non-finite values.
Results may differ from the reference program's by a relative error of at most 0.011.
Values may be sent and summed in bfloat16 or wider, within the bound.
No kernel may reach another device: no remote copies, remote signals or barrier semaphores. Data moves between devices by JAX's collectives and lax.ppermute only.
A program may use at most 64 MiB of HBM per device.

```python
import math
import jax
import jax.numpy as jnp
import numpy as np
from jax import lax

HEADS = 40
KV_HEADS = 8
HEAD_DIM = 128
TOK_DEV = 256
GROUP = 5
TOKENS = 1024
NSEQ = 2
MAXLEN = 768
N_ROW = 4


def base_rows(key, width):
    return jnp.clip(jax.random.normal(jax.random.fold_in(key, 23), (2, TOKENS, width)), -6.0, 6.0)


def draw_keys(key, part):
    width = KV_HEADS * HEAD_DIM
    draws = base_rows(jax.random.fold_in(key, 37), width)
    return draws.astype(jnp.bfloat16)


def draw_queries(key, part):
    width = HEADS * HEAD_DIM
    draws = base_rows(jax.random.fold_in(key, 31), width)
    return draws.astype(jnp.bfloat16)


def level_of(key, dims, split, low, high):
    level = 1.0
    for position, parts in split:
        steps = jax.random.uniform(jax.random.fold_in(jax.random.fold_in(key, 6), position), (parts,), jnp.float32, low / len(split), high / len(split))
        level = level * jnp.repeat(jnp.exp(steps), dims[position] // parts).reshape((-1,) + (1,) * (len(dims) - 1 - position))
    return level


def length_profile(number_of, total, bound, skew):
    weights = [(1 << 20) // math.isqrt(standing ** skew) + 1 for standing in range(2, number_of + 1)]
    surplus, counts = total - bound - (number_of - 1), [1] * (number_of - 1)
    while surplus > 0:
        candidates = [i for i in range(number_of - 1) if counts[i] < bound]
        pool, left = sum([weights[i] for i in candidates]), surplus
        for i in candidates:
            addition = min(bound - counts[i], max(1, left * weights[i] // pool), surplus)
            counts[i] = counts[i] + addition
            surplus = surplus - addition
    return np.array([bound] + counts)


def ragged(rng, number_of, total, most, slope):
    if number_of == 2:
        one = jax.random.randint(rng, (), max(1, total - most), min(most, total - 1) + 1)
        return jnp.stack([one, total - one])
    tallies = jnp.asarray(length_profile(number_of, total, most, slope), jnp.int32)
    couples = (number_of - 1) // 2
    giver, sink = tallies[1:1 + 2 * couples:2], tallies[2:2 + 2 * couples:2]
    slack = jnp.minimum(giver - 1, most - sink)
    shifted = jax.random.randint(jax.random.fold_in(rng, 1), (couples,), 0, 1 << 20) % (slack + 1)
    tallies = tallies.at[1:1 + 2 * couples:2].set(giver - shifted).at[2:2 + 2 * couples:2].set(sink + shifted)
    return tallies[jax.random.permutation(jax.random.fold_in(rng, 2), number_of)]


def gaussian(rng, dims, scale, most, pieces=(), kind=jnp.bfloat16):
    result = scale * jax.random.normal(rng, dims, jnp.float32)
    if pieces:
        result = result * level_of(rng, dims, pieces, -0.22, 0.18)
    return jnp.clip(result, -most, most).astype(kind)


def setup_inputs(seed: int = 0, part: int = 0) -> dict:
    seeds = jax.random.split(jax.random.key(seed), 5)
    part_splits = jax.random.split(jax.random.fold_in(seeds[4], part), 5)
    queries = draw_queries(jax.random.fold_in(jax.random.fold_in(seeds[4], part), 71), part)
    keys = draw_keys(jax.random.fold_in(jax.random.fold_in(seeds[4], part), 71), part)
    values = gaussian(part_splits[2], (2, TOKENS, KV_HEADS * HEAD_DIM), 1.0, 6.0, ((0, 2), (1, 4), (2, 2)))
    lengths = ragged(part_splits[3], NSEQ, TOKENS, MAXLEN, 2).astype(jnp.int32)
    return {"queries": queries, "keys": keys, "values": values, "lengths": lengths}


def rollout_begin(lengths, positions):
    finish = jnp.cumsum(lengths).astype(jnp.int32)
    return lax.optimization_barrier(jnp.sum(jnp.where(finish[None, :] <= positions[:, None], lengths[None, :], 0), axis=1)).astype(jnp.int32)

def attend(queries, keys, values, begin_at):
    padded_keys = jnp.pad(keys, ((MAXLEN, 0), (0, 0)))
    padded_values = jnp.pad(values, ((MAXLEN, 0), (0, 0)))
    window = MAXLEN + TOK_DEV
    factor = 1.0 / math.sqrt(HEAD_DIM)

    def one_block(block_id):
        offset = (block_id * TOK_DEV).astype(jnp.int32)
        query_rows = lax.dynamic_slice_in_dim(queries, offset, TOK_DEV, 0).astype(jnp.float32).reshape(TOK_DEV, KV_HEADS, GROUP, HEAD_DIM)
        key_rows = lax.dynamic_slice_in_dim(padded_keys, offset, window, 0).astype(jnp.float32).reshape(window, KV_HEADS, HEAD_DIM)
        value_rows = lax.dynamic_slice_in_dim(padded_values, offset, window, 0).astype(jnp.float32).reshape(window, KV_HEADS, HEAD_DIM)
        scores = jnp.einsum('tkgd,nkd->kgtn', query_rows, key_rows, precision=lax.Precision.HIGHEST) * factor
        query_pos = offset + jnp.arange(TOK_DEV, dtype=jnp.int32)
        key_pos = offset - MAXLEN + jnp.arange(window, dtype=jnp.int32)
        lowest = lax.dynamic_slice_in_dim(begin_at, offset, TOK_DEV, 0)
        allowed = (key_pos[None, :] >= lowest[:, None]) & (key_pos[None, :] <= query_pos[:, None])
        masked = jnp.where(allowed, scores, -jnp.inf)
        highest = lax.optimization_barrier(jnp.max(masked, axis=-1, keepdims=True))
        weights = jnp.where(allowed, jnp.exp(masked - highest), 0.0)
        summed = lax.optimization_barrier(jnp.sum(weights, axis=-1))
        rounded = lax.optimization_barrier(weights.astype(jnp.bfloat16))
        mass = rounded.astype(jnp.float32)
        mixed = jnp.einsum('kgtn,nkd->kgtd', mass, value_rows, precision=lax.Precision.HIGHEST) / summed[..., None]
        return jnp.transpose(mixed, (2, 0, 1, 3)).reshape(TOK_DEV, HEADS * HEAD_DIM).astype(jnp.bfloat16)
    blocks = lax.map(one_block, jnp.arange(N_ROW, dtype=jnp.int32))
    return blocks.reshape(TOKENS, HEADS * HEAD_DIM)

def reference(queries, keys, values, lengths):
    positions = jnp.arange(TOKENS, dtype=jnp.int32)
    begin_at = rollout_begin(lengths.astype(jnp.int32), positions)
    policy = attend(queries[0], keys[0], values[0], begin_at)
    anchor = attend(queries[1], keys[1], values[1], begin_at)
    outputs = jnp.stack([policy, anchor])
    first = policy.astype(jnp.float32).reshape(TOKENS, HEADS, HEAD_DIM)
    second = anchor.astype(jnp.float32).reshape(TOKENS, HEADS, HEAD_DIM)
    difference = first - second
    scale_sum = lax.optimization_barrier(jnp.mean(first * first, axis=-1)) + 1e-06
    gap = jnp.transpose(lax.optimization_barrier(jnp.mean(difference * difference, axis=-1)) / scale_sum)
    return (outputs, gap)
```

```python
import math

import jax
import jax.numpy as jnp
from jax import lax
from jax.experimental import pallas as pl
from jax.experimental.pallas import tpu as pltpu
from jax.sharding import PartitionSpec as P

HEADS = 40
KV_HEADS = 8
HEAD_DIM = 128


def from_behind(block, axis, distance):
    devices = range(lax.axis_size(axis))
    route = [(i - distance, i) for i in devices if i - distance in devices]
    return lax.ppermute(block, axis, route)


def swapped(block, axis, distance):
    count = lax.axis_size(axis)
    route = []
    for low in range(count):
        high = low | 1 << distance
        if high != low and high < count:
            route += [(low, high), (high, low)]
    return lax.ppermute(block, axis, route)


def relative_gap(first, second, tokens_here, heads_count):
    first = first.astype(jnp.float32).reshape(tokens_here, heads_count, HEAD_DIM)
    second = second.astype(jnp.float32).reshape(tokens_here, heads_count, HEAD_DIM)
    difference = first - second
    scale_sum = jnp.mean(first * first, axis=-1) + 1e-06
    return jnp.transpose(jnp.mean(difference * difference, axis=-1) / scale_sum)


def per_device_general(queries, keys, values, lengths):
    tokens_here = queries.shape[1]
    width_here = keys.shape[2]
    kv_local = width_here // HEAD_DIM
    group_size = HEADS // KV_HEADS
    heads_local = kv_local * group_size
    factor = 1.0 / math.sqrt(HEAD_DIM)
    row_pos = lax.axis_index("row")
    first_pos = row_pos * tokens_here
    query_pos = first_pos + jnp.arange(tokens_here, dtype=jnp.int32)
    finish = jnp.cumsum(lengths)
    begin_at = jnp.sum(
        jnp.where(finish[None, :] <= query_pos[:, None], lengths[None, :], 0), axis=1
    )
    lowest = begin_at[0]
    highest = first_pos + tokens_here - 1
    query_rows = queries[0].reshape(tokens_here, kv_local, group_size, HEAD_DIM)

    def update(running, stacked, offset):
        best, summed, accum = running
        amount = stacked.shape[1]
        key_rows = stacked[0].reshape(amount, kv_local, HEAD_DIM)
        value_rows = stacked[1].reshape(amount, kv_local, HEAD_DIM)
        scores = (
            jnp.einsum("tkgd,nkd->kgtn", query_rows, key_rows, preferred_element_type=jnp.float32)
            * factor
        )
        key_pos = offset + jnp.arange(amount, dtype=jnp.int32)
        allowed = (key_pos[None, :] >= begin_at[:, None]) & (key_pos[None, :] <= query_pos[:, None])
        masked = jnp.where(allowed, scores, -jnp.inf)
        fresh_best = jnp.maximum(best, jnp.max(masked, axis=-1))
        weights = jnp.where(allowed, jnp.exp(masked - fresh_best[..., None]), 0.0)
        shrink = jnp.exp(best - fresh_best)
        summed = summed * shrink + jnp.sum(weights, axis=-1)
        accum = accum * shrink[..., None] + jnp.einsum(
            "kgtn,nkd->kgtd",
            weights.astype(jnp.bfloat16),
            value_rows,
            preferred_element_type=jnp.float32,
        )
        return (fresh_best, summed, accum)

    def absorb(running, stacked, offset):
        amount = stacked.shape[1]
        needed = (offset + amount > lowest) & (offset <= highest)
        return lax.cond(
            needed, lambda inner: update(inner, stacked, offset), lambda inner: inner, running
        )

    start_state = (
        jnp.full((kv_local, group_size, tokens_here), -1e30, jnp.float32),
        jnp.zeros((kv_local, group_size, tokens_here), jnp.float32),
        jnp.zeros((kv_local, group_size, tokens_here, HEAD_DIM), jnp.float32),
    )
    paired = jnp.concatenate([keys, values], axis=0)
    reach = lax.axis_size("row") // 2 + 1
    running = absorb(start_state, paired, first_pos)

    def advance(step_id, loop_state):
        inner, moving = loop_state
        moving = from_behind(moving, "row", 1)
        return (absorb(inner, moving, (row_pos - step_id) * tokens_here), moving)

    running, _ = lax.fori_loop(1, reach + 1, advance, (running, paired))
    _, summed, accum = running
    mixed = accum / summed[..., None]
    outputs = (
        jnp.transpose(mixed, (2, 0, 1, 3))
        .reshape(tokens_here, heads_local * HEAD_DIM)
        .astype(jnp.bfloat16)[None]
    )
    half_heads = heads_local // 2
    partner = swapped(outputs, "mp", 0)
    model_pos = lax.axis_index("mp")
    is_policy = model_pos == 0
    policy = jnp.where(is_policy, outputs[0], partner[0])
    anchor = jnp.where(is_policy, partner[0], outputs[0])
    column_at = model_pos * half_heads * HEAD_DIM
    policy_part = lax.dynamic_slice_in_dim(policy, column_at, half_heads * HEAD_DIM, 1)
    anchor_part = lax.dynamic_slice_in_dim(anchor, column_at, half_heads * HEAD_DIM, 1)
    gap = relative_gap(policy_part, anchor_part, tokens_here, half_heads)
    return (outputs, gap)


SCALE = math.log2(math.e) / math.sqrt(HEAD_DIM)
GROUP = HEADS // KV_HEADS
NT = (((1,), (1,)), ((), ()))
VMEM = pl.BlockSpec(memory_space=pltpu.VMEM)
SMEM = pl.BlockSpec(memory_space=pltpu.SMEM)
HBM = pl.BlockSpec(memory_space=pltpu.HBM)


def lanes(index, width):
    if isinstance(index, int):
        return pl.ds(index * width, width)
    return pl.ds(pl.multiple_of(index * width, width), width)


def twice(part):
    return jnp.concatenate([part, part], axis=1)


def weights_of(scores, top):
    return jnp.exp2(scores * SCALE - top * SCALE)


def with_ones(value_rows):
    return jnp.concatenate([value_rows, jnp.ones_like(value_rows)], axis=1)


def scores_of(query_rows, key_rows):
    return lax.dot_general(query_rows, key_rows, NT, preferred_element_type=jnp.float32)


def diagonal_kernel(
    len_ref, q_hbm, k_hbm, v_hbm, q_ref, acc_ref, top_ref, near_ref, far_ref, k_ref, v_ref, sem
):
    tokens_here = q_ref.shape[0]
    half = tokens_here // 2
    kv_local = k_ref.shape[1] // HEAD_DIM
    copies = [
        pltpu.make_async_copy(k_hbm.at[0], k_ref, sem.at[0]),
        pltpu.make_async_copy(v_hbm.at[0], v_ref, sem.at[1]),
    ]
    for kv in range(kv_local):
        cols = lanes(kv, GROUP * HEAD_DIM)
        copies.append(
            pltpu.make_async_copy(q_hbm.at[0, :, cols], q_ref.at[:, cols], sem.at[2 + kv])
        )
    for copy in (copies[0], copies[2], copies[1], *copies[3:]):
        copy.start()
    boundary = len_ref[0] - lax.axis_index("row") * tokens_here
    query = lax.broadcasted_iota(jnp.int32, (tokens_here, tokens_here), 0)
    key = lax.broadcasted_iota(jnp.int32, (tokens_here, tokens_here), 1)
    for hops, ref in ((1, near_ref), (2, far_ref)):
        exists = lax.axis_index("row") >= hops
        kept = (query < boundary) | (key - hops * tokens_here >= boundary)
        ref[...] = jnp.where(kept & exists, 0.0, -jnp.inf)
    kept = (key <= query) & ((query < boundary) | (key >= boundary))
    bias = jnp.where(kept, 0.0, -jnp.inf)
    copies[0].wait()
    for kv in range(kv_local):
        copies[2 + kv].wait()
        if kv == 0:
            copies[1].wait()
        key_rows = k_ref[:, lanes(kv, HEAD_DIM)]
        value_rows = with_ones(v_ref[:, lanes(kv, HEAD_DIM)])
        for g in range(GROUP):
            head = kv * GROUP + g
            for low in (0, half):
                rows = pl.ds(low, half)
                seen = low + half
                scores = scores_of(q_ref[rows, lanes(head, HEAD_DIM)], key_rows[:seen])
                scores += bias[low:seen, :seen]
                top = jnp.max(scores, axis=1, keepdims=True)
                mass = weights_of(scores, top).astype(jnp.bfloat16)
                acc_ref[rows, lanes(head, 2 * HEAD_DIM)] = jnp.dot(
                    mass, value_rows[:seen], preferred_element_type=jnp.float32
                )
                top_ref[rows, lanes(head, HEAD_DIM)] = jnp.broadcast_to(top, (half, HEAD_DIM))


def absorb(query_rows, key_rows, value_rows, bias, old_acc, old_top):
    scores = scores_of(query_rows, key_rows) + bias
    top = jnp.maximum(old_top, jnp.max(scores, axis=1, keepdims=True))
    mass = weights_of(scores, twice(top)).astype(jnp.bfloat16)
    part = jnp.dot(mass, value_rows, preferred_element_type=jnp.float32)
    return old_acc * twice(weights_of(old_top, top)) + part, top


def near_kernel(own, q_ref, kv_ref, acc_in, top_in, bias_ref, acc_ref, top_ref):
    mp = lax.axis_index("mp")
    heads_half = top_ref.shape[1] // HEAD_DIM
    first_head = (mp if own else 1 - mp) * heads_half
    bias = bias_ref[...]
    for local in range(heads_half):
        kv = local // GROUP
        if local % GROUP == 0:
            key_rows = kv_ref[0, :, lanes(kv, HEAD_DIM)]
            value_rows = with_ones(kv_ref[1, :, lanes(kv, HEAD_DIM)])
        head = first_head + local
        acc, top = absorb(
            q_ref[:, lanes(head, HEAD_DIM)],
            key_rows,
            value_rows,
            bias,
            acc_in[:, lanes(head, 2 * HEAD_DIM)],
            top_in[:, lanes(head, HEAD_DIM)],
        )
        acc_ref[:, lanes(local, 2 * HEAD_DIM)] = acc
        top_ref[:, lanes(local, HEAD_DIM)] = top


def far_heads(first_head, q_ref, kv_ref, acc_ref, top_ref, bias_ref, store):
    bias = bias_ref[...]
    for local in range(top_ref.shape[1] // HEAD_DIM):
        kv = local // GROUP
        if local % GROUP == 0:
            key_rows = kv_ref[0, :, lanes(kv, HEAD_DIM)]
            value_rows = with_ones(kv_ref[1, :, lanes(kv, HEAD_DIM)])
        acc, _ = absorb(
            q_ref[:, lanes(first_head + local, HEAD_DIM)],
            key_rows,
            value_rows,
            bias,
            acc_ref[:, lanes(local, 2 * HEAD_DIM)],
            top_ref[:, lanes(local, HEAD_DIM)],
        )
        store(local, (acc[:, :HEAD_DIM] / acc[:, HEAD_DIM:]).astype(jnp.bfloat16))


def far_other_kernel(q_ref, kv_ref, acc_ref, top_ref, bias_ref, out_ref):
    heads_half = out_ref.shape[2] // HEAD_DIM

    def store(local, block):
        out_ref[0, :, lanes(local, HEAD_DIM)] = block

    first_head = (1 - lax.axis_index("mp")) * heads_half
    far_heads(first_head, q_ref, kv_ref, acc_ref, top_ref, bias_ref, store)


def far_own_kernel(
    q_ref, kv_ref, acc_ref, top_ref, bias_ref, sent_ref, got_ref, out_ref, gap_ref, mine_ref, sem
):
    width = sent_ref.shape[2]
    heads_half = width // HEAD_DIM
    mp = lax.axis_index("mp")
    copies = [
        pltpu.make_async_copy(sent_ref.at[0], out_ref.at[0, :, lanes(1 - mp, width)], sem.at[0])
    ]
    copies[0].start()
    mean = jnp.full((16, HEAD_DIM), 1.0 / HEAD_DIM, jnp.bfloat16)

    def store(local, block):
        mine_ref[:, lanes(local, HEAD_DIM)] = block
        if local % GROUP == GROUP - 1:
            step = local // GROUP
            cols = lanes(step, GROUP * HEAD_DIM)
            spot = lanes(mp * (heads_half // GROUP) + step, GROUP * HEAD_DIM)
            copy = pltpu.make_async_copy(
                mine_ref.at[:, cols], out_ref.at[0, :, spot], sem.at[1 + step]
            )
            copy.start()
            copies.append(copy)
        mine = block.astype(jnp.float32)
        theirs = got_ref[0, :, lanes(local, HEAD_DIM)].astype(jnp.float32)
        difference = mine - theirs
        policy = jnp.where(mp == 0, mine, theirs)
        squares = jnp.concatenate([difference * difference, policy * policy], axis=0)
        means = scores_of(mean, squares.astype(jnp.bfloat16))
        tokens_here = block.shape[0]
        gap_ref[local : local + 1, :] = means[:1, :tokens_here] / (
            means[:1, tokens_here:] + 1e-06
        )

    far_heads(mp * heads_half, q_ref, kv_ref, acc_ref, top_ref, bias_ref, store)
    for copy in copies:
        copy.wait()


def call(kernel, out_shape, in_specs, out_specs, flops, **more):
    return pl.pallas_call(
        kernel,
        out_shape=out_shape,
        in_specs=in_specs,
        out_specs=out_specs,
        cost_estimate=pl.CostEstimate(
            flops=int(flops), bytes_accessed=4 << 20, transcendentals=0
        ),
        compiler_params=pltpu.CompilerParams(vmem_limit_bytes=16 * 2**20),
        **more,
    )


def per_device_paired(queries, keys, values, lengths):
    tokens_here = queries.shape[1]
    kv_local = keys.shape[2] // HEAD_DIM
    heads_local = kv_local * GROUP
    width = heads_local * HEAD_DIM
    half = width // 2
    half_kv = keys.shape[2] // 2
    count = lax.axis_size("row")
    mp = lax.axis_index("mp")
    f32, bf16 = jnp.float32, jnp.bfloat16
    shape = jax.ShapeDtypeStruct
    bias_type = shape((tokens_here, tokens_here), f32)
    work = 8 * heads_local * tokens_here * tokens_here * HEAD_DIM

    def pack(which):
        parts = [lax.dynamic_slice_in_dim(x, which * half_kv, half_kv, 2) for x in (keys, values)]
        return jnp.concatenate(parts, axis=0)

    near_route = [(i - 1, i) for i in range(1, count)]
    far_route = [(i - 1, i) for i in range(2, count)]
    other_near = lax.ppermute(pack(1 - mp), "row", near_route)
    own_near = lax.ppermute(pack(mp), "row", near_route)
    query_rows, acc, top, near_bias, far_bias = call(
        diagonal_kernel,
        (
            shape((tokens_here, width), bf16),
            shape((tokens_here, 2 * width), f32),
            shape((tokens_here, width), f32),
            bias_type,
            bias_type,
        ),
        [SMEM] + [HBM] * 3,
        [VMEM] * 5,
        work,
        scratch_shapes=[
            pltpu.VMEM((tokens_here, keys.shape[2]), bf16),
            pltpu.VMEM((tokens_here, keys.shape[2]), bf16),
            pltpu.SemaphoreType.DMA((2 + kv_local,)),
        ],
    )(lengths, queries, keys, values)
    other_far = lax.ppermute(other_near, "row", far_route)
    state_type = (shape((tokens_here, width), f32), shape((tokens_here, half), f32))

    def near(own, block):
        return call(
            lambda *refs: near_kernel(own, *refs), state_type, [VMEM] * 5, [VMEM] * 2, work
        )(query_rows, block, acc, top, near_bias)

    other_state = near(False, other_near)
    own_far = lax.ppermute(own_near, "row", far_route)
    own_state = near(True, own_near)
    sent = call(
        far_other_kernel, shape((1, tokens_here, half), bf16), [VMEM] * 5, VMEM, work
    )(query_rows, other_far, *other_state, far_bias)
    got = lax.ppermute(sent, "mp", [(0, 1), (1, 0)])
    outputs, gap = call(
        far_own_kernel,
        (
            shape((1, tokens_here, width), bf16),
            shape((heads_local // 2, tokens_here), f32),
        ),
        [VMEM] * 7,
        [HBM, VMEM],
        work,
        scratch_shapes=[
            pltpu.VMEM((tokens_here, half), bf16),
            pltpu.SemaphoreType.DMA((1 + kv_local // 2,)),
        ],
    )(query_rows, own_far, *own_state, far_bias, sent, got)
    return (outputs, gap)


def two_hops(mesh, rollouts):
    return rollouts == 2 and mesh.shape["row"] // 2 == 2 and mesh.shape["mp"] == 2


def solution(mesh):
    in_specs = (
        P("mp", ("groups", "row"), "col"),
        P("mp", ("groups", "row"), "col"),
        P("mp", ("groups", "row"), "col"),
        P("groups"),
    )
    out_specs = (P("mp", ("groups", "row"), "col"), P(("col", "mp"), ("groups", "row")))

    def place(body):
        return jax.shard_map(
            body, mesh=mesh, in_specs=in_specs, out_specs=out_specs, check_vma=False
        )

    def step(queries, keys, values, lengths):
        rollouts = lengths.shape[0] // mesh.shape["groups"]
        kv_local = keys.shape[2] // HEAD_DIM // mesh.shape["col"]
        if not two_hops(mesh, rollouts) or kv_local % 2:
            return place(per_device_general)(queries, keys, values, lengths)
        return place(per_device_paired)(queries, keys, values, lengths)

    return step
```

```python
import math

import jax
import jax.numpy as jnp
from jax import lax
from jax.experimental import pallas as pl
from jax.experimental.pallas import tpu as pltpu
from jax.sharding import PartitionSpec as P

HEADS = 40
KV_HEADS = 8
HEAD_DIM = 128


def from_behind(block, axis, distance):
    devices = range(lax.axis_size(axis))
    route = [(i - distance, i) for i in devices if i - distance in devices]
    return lax.ppermute(block, axis, route)


def swapped(block, axis, distance):
    count = lax.axis_size(axis)
    route = []
    for low in range(count):
        high = low | 1 << distance
        if high != low and high < count:
            route += [(low, high), (high, low)]
    return lax.ppermute(block, axis, route)


def relative_gap(first, second, tokens_here, heads_count):
    first = first.astype(jnp.float32).reshape(tokens_here, heads_count, HEAD_DIM)
    second = second.astype(jnp.float32).reshape(tokens_here, heads_count, HEAD_DIM)
    difference = first - second
    scale_sum = jnp.mean(first * first, axis=-1) + 1e-06
    return jnp.transpose(jnp.mean(difference * difference, axis=-1) / scale_sum)


def per_device_general(queries, keys, values, lengths):
    tokens_here = queries.shape[1]
    width_here = keys.shape[2]
    kv_local = width_here // HEAD_DIM
    group_size = HEADS // KV_HEADS
    heads_local = kv_local * group_size
    factor = 1.0 / math.sqrt(HEAD_DIM)
    row_pos = lax.axis_index("row")
    first_pos = row_pos * tokens_here
    query_pos = first_pos + jnp.arange(tokens_here, dtype=jnp.int32)
    finish = jnp.cumsum(lengths)
    begin_at = jnp.sum(
        jnp.where(finish[None, :] <= query_pos[:, None], lengths[None, :], 0), axis=1
    )
    lowest = begin_at[0]
    highest = first_pos + tokens_here - 1
    query_rows = queries[0].reshape(tokens_here, kv_local, group_size, HEAD_DIM)

    def update(running, stacked, offset):
        best, summed, accum = running
        amount = stacked.shape[1]
        key_rows = stacked[0].reshape(amount, kv_local, HEAD_DIM)
        value_rows = stacked[1].reshape(amount, kv_local, HEAD_DIM)
        scores = (
            jnp.einsum("tkgd,nkd->kgtn", query_rows, key_rows, preferred_element_type=jnp.float32)
            * factor
        )
        key_pos = offset + jnp.arange(amount, dtype=jnp.int32)
        allowed = (key_pos[None, :] >= begin_at[:, None]) & (key_pos[None, :] <= query_pos[:, None])
        masked = jnp.where(allowed, scores, -jnp.inf)
        fresh_best = jnp.maximum(best, jnp.max(masked, axis=-1))
        weights = jnp.where(allowed, jnp.exp(masked - fresh_best[..., None]), 0.0)
        shrink = jnp.exp(best - fresh_best)
        summed = summed * shrink + jnp.sum(weights, axis=-1)
        accum = accum * shrink[..., None] + jnp.einsum(
            "kgtn,nkd->kgtd",
            weights.astype(jnp.bfloat16),
            value_rows,
            preferred_element_type=jnp.float32,
        )
        return (fresh_best, summed, accum)

    def absorb(running, stacked, offset):
        amount = stacked.shape[1]
        needed = (offset + amount > lowest) & (offset <= highest)
        return lax.cond(
            needed, lambda inner: update(inner, stacked, offset), lambda inner: inner, running
        )

    start_state = (
        jnp.full((kv_local, group_size, tokens_here), -1e30, jnp.float32),
        jnp.zeros((kv_local, group_size, tokens_here), jnp.float32),
        jnp.zeros((kv_local, group_size, tokens_here, HEAD_DIM), jnp.float32),
    )
    paired = jnp.concatenate([keys, values], axis=0)
    reach = lax.axis_size("row") // 2 + 1
    running = absorb(start_state, paired, first_pos)

    def advance(step_id, loop_state):
        inner, moving = loop_state
        moving = from_behind(moving, "row", 1)
        return (absorb(inner, moving, (row_pos - step_id) * tokens_here), moving)

    running, _ = lax.fori_loop(1, reach + 1, advance, (running, paired))
    _, summed, accum = running
    mixed = accum / summed[..., None]
    outputs = (
        jnp.transpose(mixed, (2, 0, 1, 3))
        .reshape(tokens_here, heads_local * HEAD_DIM)
        .astype(jnp.bfloat16)[None]
    )
    half_heads = heads_local // 2
    partner = swapped(outputs, "mp", 0)
    model_pos = lax.axis_index("mp")
    is_policy = model_pos == 0
    policy = jnp.where(is_policy, outputs[0], partner[0])
    anchor = jnp.where(is_policy, partner[0], outputs[0])
    column_at = model_pos * half_heads * HEAD_DIM
    policy_part = lax.dynamic_slice_in_dim(policy, column_at, half_heads * HEAD_DIM, 1)
    anchor_part = lax.dynamic_slice_in_dim(anchor, column_at, half_heads * HEAD_DIM, 1)
    gap = relative_gap(policy_part, anchor_part, tokens_here, half_heads)
    return (outputs, gap)


SCALE = math.log2(math.e) / math.sqrt(HEAD_DIM)
GROUP = HEADS // KV_HEADS
BIG = 2.0**100
LIMIT = 2.0**100
NT = (((1,), (1,)), ((), ()))
VMEM = pl.BlockSpec(memory_space=pltpu.VMEM)
SMEM = pl.BlockSpec(memory_space=pltpu.SMEM)
HBM = pl.BlockSpec(memory_space=pltpu.HBM)


def lanes(index, width):
    if isinstance(index, int):
        return pl.ds(index * width, width)
    return pl.ds(pl.multiple_of(index * width, width), width)


def with_ones(value_rows):
    return jnp.concatenate([value_rows, jnp.ones_like(value_rows)], axis=1)


def scores_of(query_rows, key_rows):
    return lax.dot_general(query_rows, key_rows, NT, preferred_element_type=jnp.float32)


def mass_of(scores):
    return jnp.exp2(scores * SCALE).astype(jnp.bfloat16)


def spread(mass, value_rows):
    return jnp.dot(mass, value_rows, preferred_element_type=jnp.float32)


def in_columns(shape, *columns):
    lane = lax.broadcasted_iota(jnp.int32, shape, 1)
    tile = jnp.zeros(shape, jnp.float32)
    for index, column in enumerate(columns):
        tile = jnp.where(lane == index, column, tile)
    return tile


def diagonal_kernel(
    len_hbm, q_hbm, other_ref, own_ref, wide_ref, acc_ref, near_ref, far_ref, bias_ref, q_ref,
    len_ref, sem
):
    tokens_here = q_ref.shape[0]
    half = tokens_here // 2
    mp = lax.axis_index("mp")
    row_pos = lax.axis_index("row")
    kv_half = other_ref.shape[2] // HEAD_DIM
    spot = GROUP * HEAD_DIM
    len_copy = pltpu.make_async_copy(len_hbm, len_ref, sem.at[2 * kv_half])
    len_copy.start()
    copies = []
    for step in range(2 * kv_half):
        which = 1 - mp if step < kv_half else mp
        copies.append(
            pltpu.make_async_copy(
                q_hbm.at[0, :, lanes(which * kv_half + step % kv_half, spot)],
                q_ref.at[:, lanes(step, spot)],
                sem.at[step],
            )
        )
        copies[step].start()
    len_copy.wait()
    boundary = len_ref[0] - row_pos * tokens_here
    query = lax.broadcasted_iota(jnp.int32, (tokens_here, tokens_here), 0)
    key = lax.broadcasted_iota(jnp.int32, (tokens_here, tokens_here), 1)
    kept = (key <= query) & ((query < boundary) | (key >= boundary))
    bias_ref[...] = jnp.where(kept, 0.0, -jnp.inf)
    tile = (tokens_here, HEAD_DIM)
    token = lax.broadcasted_iota(jnp.int32, tile, 0)
    for hops, ref in ((1, near_ref), (2, far_ref)):
        gone = jnp.where(row_pos >= hops, 0.0, -BIG)
        before = jnp.where(token - hops * tokens_here < boundary, -BIG, 0.0)
        ref[...] = in_columns(tile, -1.0, before, gone).astype(jnp.bfloat16)
    later = in_columns(tile, 0.0, jnp.where(token >= boundary, 1.0, 0.0), 1.0)
    first_lane = lax.broadcasted_iota(jnp.int32, (half, HEAD_DIM), 1) == 0
    for step in range(2 * kv_half):
        copies[step].wait()
        pack_ref = other_ref if step < kv_half else own_ref
        key_rows = pack_ref[0, :, lanes(step % kv_half, HEAD_DIM)]
        value_rows = value_of(pack_ref, step % kv_half)
        for g in range(GROUP):
            local = step * GROUP + g
            for low in (0, half):
                rows = pl.ds(low, half)
                seen = low + half
                query_rows = q_ref[rows, lanes(local, HEAD_DIM)]
                scores = scores_of(query_rows, key_rows[:seen]) + bias_ref[rows, :seen]
                top = jnp.max(scores, axis=1, keepdims=True).astype(jnp.bfloat16)
                top = top.astype(jnp.float32)
                acc_ref[rows, lanes(local, 2 * HEAD_DIM)] = spread(
                    mass_of(scores - top), value_rows[:seen]
                )
                extra = jnp.where(first_lane, top, later[low:seen]).astype(jnp.bfloat16)
                wide_ref[rows, lanes(2 * local, HEAD_DIM)] = query_rows
                wide_ref[rows, lanes(2 * local + 1, HEAD_DIM)] = extra


def key_of(kv_ref, kv, tile_ref):
    return jnp.concatenate([kv_ref[0, :, lanes(kv, HEAD_DIM)], tile_ref[...]], axis=1)


def value_of(kv_ref, kv):
    return with_ones(kv_ref[1, :, lanes(kv, HEAD_DIM)])


def near_kernel(own, wide_ref, kv_ref, acc_in, tile_ref, acc_ref):
    heads_half = acc_ref.shape[1] // (2 * HEAD_DIM)
    first_head = heads_half if own else 0
    for local in range(heads_half):
        if local % GROUP == 0:
            key_rows = key_of(kv_ref, local // GROUP, tile_ref)
            value_rows = value_of(kv_ref, local // GROUP)
        cols = lanes(first_head + local, 2 * HEAD_DIM)
        mass = mass_of(scores_of(wide_ref[:, cols], key_rows))
        acc_ref[:, lanes(local, 2 * HEAD_DIM)] = acc_in[:, cols] + spread(mass, value_rows)


def far_heads(first_head, refs, store):
    wide_ref, _, far_kv, _, acc_ref, _, far_tile = refs
    worst = None
    for local in range(acc_ref.shape[1] // (2 * HEAD_DIM)):
        if local % GROUP == 0:
            key_rows = key_of(far_kv, local // GROUP, far_tile)
            value_rows = value_of(far_kv, local // GROUP)
        mass = mass_of(scores_of(wide_ref[:, lanes(first_head + local, 2 * HEAD_DIM)], key_rows))
        acc = acc_ref[:, lanes(local, 2 * HEAD_DIM)] + spread(mass, value_rows)
        total = acc[:, HEAD_DIM:]
        store(local, (acc[:, :HEAD_DIM] / total).astype(jnp.bfloat16))
        worst = total if worst is None else jnp.maximum(worst, total)
    return jnp.logical_not(jnp.max(worst) < LIMIT)


def far_heads_again(first_head, refs, store):
    wide_ref, near_kv, far_kv, first_ref, acc_ref, near_tile, far_tile = refs

    @pl.loop(0, acc_ref.shape[1] // (2 * HEAD_DIM))
    def _(local):
        cols = lanes(first_head + local, 2 * HEAD_DIM)
        query_rows = wide_ref[:, cols]
        kv = local // GROUP
        near_scores = scores_of(query_rows, key_of(near_kv, kv, near_tile))
        far_scores = scores_of(query_rows, key_of(far_kv, kv, far_tile))
        top = jnp.max(jnp.maximum(near_scores, far_scores), axis=1, keepdims=True)
        top = jnp.maximum(top, 0.0)
        acc = (
            first_ref[:, cols] * jnp.exp2(-top * SCALE)
            + spread(mass_of(near_scores - top), value_of(near_kv, kv))
            + spread(mass_of(far_scores - top), value_of(far_kv, kv))
        )
        store(local, (acc[:, :HEAD_DIM] / acc[:, HEAD_DIM:]).astype(jnp.bfloat16))


def far_other_kernel(*refs):
    refs, out_ref = refs[:7], refs[7]
    first_head = 0

    def store(local, block):
        out_ref[0, :, lanes(local, HEAD_DIM)] = block

    too_high = far_heads(first_head, refs, store)

    @pl.when(too_high)
    def _():
        far_heads_again(first_head, refs, store)


def far_own_kernel(*refs):
    refs, (sent_ref, got_ref, out_ref, gap_ref, mine_ref, sem) = refs[:7], refs[7:]
    width = sent_ref.shape[2]
    tokens_here = sent_ref.shape[1]
    heads_half = width // HEAD_DIM
    mp = lax.axis_index("mp")
    first_head = heads_half
    spot = GROUP * HEAD_DIM
    steps = heads_half // GROUP
    sent_copy = pltpu.make_async_copy(
        sent_ref.at[0], out_ref.at[0, :, lanes(1 - mp, width)], sem.at[steps]
    )
    sent_copy.start()
    mine_copies = [
        pltpu.make_async_copy(
            mine_ref.at[:, lanes(step, spot)],
            out_ref.at[0, :, lanes(mp * steps + step, spot)],
            sem.at[step],
        )
        for step in range(steps)
    ]
    lane = lax.broadcasted_iota(jnp.int32, (tokens_here, HEAD_DIM), 1)
    state = {"far": jnp.zeros((tokens_here, HEAD_DIM), jnp.float32)}
    state["size"] = state["far"]

    def squares(local, block):
        mine = block.astype(jnp.float32)
        theirs = got_ref[0, :, lanes(local, HEAD_DIM)].astype(jnp.float32)
        difference = mine - theirs
        policy = jnp.where(mp == 0, mine, theirs)
        return (
            jnp.sum(difference * difference, axis=1, keepdims=True),
            jnp.sum(policy * policy, axis=1, keepdims=True),
        )

    def gap_of(far, size):
        return far.T[:heads_half] / HEAD_DIM / (size.T[:heads_half] / HEAD_DIM + 1e-06)

    def store(local, block):
        mine_ref[:, lanes(local, HEAD_DIM)] = block
        if local % GROUP == GROUP - 1:
            mine_copies[local // GROUP].start()
        far, size = squares(local, block)
        state["far"] = jnp.where(lane == local, far, state["far"])
        state["size"] = jnp.where(lane == local, size, state["size"])

    too_high = far_heads(first_head, refs, store)
    gap_ref[...] = gap_of(state["far"], state["size"])
    sent_copy.wait()
    for copy in mine_copies:
        copy.wait()

    @pl.when(too_high)
    def _():
        def store_again(local, block):
            mine_ref[:, lanes(local, HEAD_DIM)] = block

        far_heads_again(first_head, refs, store_again)
        far = size = jnp.zeros((tokens_here, HEAD_DIM), jnp.float32)
        for local in range(heads_half):
            parts = squares(local, mine_ref[:, lanes(local, HEAD_DIM)])
            far = jnp.where(lane == local, parts[0], far)
            size = jnp.where(lane == local, parts[1], size)
        gap_ref[...] = gap_of(far, size)
        for copy in mine_copies:
            copy.start()
        for copy in mine_copies:
            copy.wait()


def in_hbm(array):
    return pltpu.with_memory_space_constraint(array, pltpu.HBM)


def call(kernel, out_shape, in_specs, out_specs, flops, vmem_mib=16, **more):
    return pl.pallas_call(
        kernel,
        out_shape=out_shape,
        in_specs=in_specs,
        out_specs=out_specs,
        cost_estimate=pl.CostEstimate(
            flops=int(flops), bytes_accessed=4 << 20, transcendentals=0
        ),
        compiler_params=pltpu.CompilerParams(vmem_limit_bytes=vmem_mib * 2**20),
        **more,
    )


def per_device_paired(queries, keys, values, lengths):
    tokens_here = queries.shape[1]
    kv_local = keys.shape[2] // HEAD_DIM
    heads_local = kv_local * GROUP
    width = heads_local * HEAD_DIM
    half = width // 2
    half_kv = keys.shape[2] // 2
    count = lax.axis_size("row")
    mp = lax.axis_index("mp")
    f32, bf16 = jnp.float32, jnp.bfloat16
    shape = jax.ShapeDtypeStruct
    tile_type = shape((tokens_here, HEAD_DIM), bf16)
    work = 8 * heads_local * tokens_here * tokens_here * HEAD_DIM

    def pack(which):
        parts = [lax.dynamic_slice_in_dim(x, which * half_kv, half_kv, 2) for x in (keys, values)]
        return jnp.concatenate(parts, axis=0)

    near_route = [(i - 1, i) for i in range(1, count)]
    far_route = [(i - 1, i) for i in range(2, count)]
    other = pack(1 - mp)
    other_near = lax.ppermute(other, "row", near_route)
    other, which = lax.optimization_barrier((other, mp))
    own = pack(which)
    own_near = lax.ppermute(own, "row", near_route)
    wide, acc, near_tile, far_tile = call(
        diagonal_kernel,
        (
            shape((tokens_here, 2 * width), bf16),
            shape((tokens_here, 2 * width), f32),
            tile_type,
            tile_type,
        ),
        [HBM] * 2 + [VMEM] * 2,
        [VMEM] * 4,
        work,
        vmem_mib=16,
        scratch_shapes=[
            pltpu.VMEM((tokens_here, tokens_here), f32),
            pltpu.VMEM((tokens_here, width), bf16),
            pltpu.SMEM(lengths.shape, jnp.int32),
            pltpu.SemaphoreType.DMA((1 + kv_local,)),
        ],
    )(in_hbm(lengths), in_hbm(queries), other, own)
    other_far = lax.ppermute(other_near, "row", far_route)

    def near(own, block):
        return call(
            lambda *refs: near_kernel(own, *refs),
            shape((tokens_here, width), f32),
            [VMEM] * 4,
            VMEM,
            work,
        )(wide, block, acc, near_tile)

    other_acc = near(False, other_near)
    own_far = lax.ppermute(own_near, "row", far_route)
    own_acc = near(True, own_near)
    sent = call(
        far_other_kernel, shape((1, tokens_here, half), bf16), [VMEM] * 7, VMEM, work
    )(wide, other_near, other_far, acc, other_acc, near_tile, far_tile)
    got = lax.ppermute(sent, "mp", [(0, 1), (1, 0)])
    outputs, gap = call(
        far_own_kernel,
        (
            shape((1, tokens_here, width), bf16),
            shape((heads_local // 2, tokens_here), f32),
        ),
        [VMEM] * 9,
        [HBM, VMEM],
        work,
        scratch_shapes=[
            pltpu.VMEM((tokens_here, half), bf16),
            pltpu.SemaphoreType.DMA((1 + kv_local // 2,)),
        ],
    )(wide, own_near, own_far, acc, own_acc, near_tile, far_tile, sent, got)
    return (outputs, gap)


def two_hops(mesh, rollouts):
    return rollouts == 2 and mesh.shape["row"] // 2 == 2 and mesh.shape["mp"] == 2


def solution(mesh):
    in_specs = (
        P("mp", ("groups", "row"), "col"),
        P("mp", ("groups", "row"), "col"),
        P("mp", ("groups", "row"), "col"),
        P("groups"),
    )
    out_specs = (P("mp", ("groups", "row"), "col"), P(("col", "mp"), ("groups", "row")))

    def place(body):
        return jax.shard_map(
            body, mesh=mesh, in_specs=in_specs, out_specs=out_specs, check_vma=False
        )

    def step(queries, keys, values, lengths):
        rollouts = lengths.shape[0] // mesh.shape["groups"]
        kv_local = keys.shape[2] // HEAD_DIM // mesh.shape["col"]
        if not two_hops(mesh, rollouts) or kv_local % 2:
            return place(per_device_general)(queries, keys, values, lengths)
        return place(per_device_paired)(queries, keys, values, lengths)

    return step
```

```python
import math

import jax
import jax.numpy as jnp
from jax import lax
from jax.experimental import pallas as pl
from jax.experimental.pallas import tpu as pltpu
from jax.sharding import PartitionSpec as P

HEADS = 40
KV_HEADS = 8
HEAD_DIM = 128


def from_behind(block, axis, distance):
    devices = range(lax.axis_size(axis))
    route = [(i - distance, i) for i in devices if i - distance in devices]
    return lax.ppermute(block, axis, route)


def swapped(block, axis, distance):
    count = lax.axis_size(axis)
    route = []
    for low in range(count):
        high = low | 1 << distance
        if high != low and high < count:
            route += [(low, high), (high, low)]
    return lax.ppermute(block, axis, route)


def relative_gap(first, second, tokens_here, heads_count):
    first = first.astype(jnp.float32).reshape(tokens_here, heads_count, HEAD_DIM)
    second = second.astype(jnp.float32).reshape(tokens_here, heads_count, HEAD_DIM)
    difference = first - second
    scale_sum = jnp.mean(first * first, axis=-1) + 1e-06
    return jnp.transpose(jnp.mean(difference * difference, axis=-1) / scale_sum)


def per_device_general(queries, keys, values, lengths):
    tokens_here = queries.shape[1]
    width_here = keys.shape[2]
    kv_local = width_here // HEAD_DIM
    group_size = HEADS // KV_HEADS
    heads_local = kv_local * group_size
    factor = 1.0 / math.sqrt(HEAD_DIM)
    row_pos = lax.axis_index("row")
    first_pos = row_pos * tokens_here
    query_pos = first_pos + jnp.arange(tokens_here, dtype=jnp.int32)
    finish = jnp.cumsum(lengths)
    begin_at = jnp.sum(
        jnp.where(finish[None, :] <= query_pos[:, None], lengths[None, :], 0), axis=1
    )
    lowest = begin_at[0]
    highest = first_pos + tokens_here - 1
    query_rows = queries[0].reshape(tokens_here, kv_local, group_size, HEAD_DIM)

    def update(running, stacked, offset):
        best, summed, accum = running
        amount = stacked.shape[1]
        key_rows = stacked[0].reshape(amount, kv_local, HEAD_DIM)
        value_rows = stacked[1].reshape(amount, kv_local, HEAD_DIM)
        scores = (
            jnp.einsum("tkgd,nkd->kgtn", query_rows, key_rows, preferred_element_type=jnp.float32)
            * factor
        )
        key_pos = offset + jnp.arange(amount, dtype=jnp.int32)
        allowed = (key_pos[None, :] >= begin_at[:, None]) & (key_pos[None, :] <= query_pos[:, None])
        masked = jnp.where(allowed, scores, -jnp.inf)
        fresh_best = jnp.maximum(best, jnp.max(masked, axis=-1))
        weights = jnp.where(allowed, jnp.exp(masked - fresh_best[..., None]), 0.0)
        shrink = jnp.exp(best - fresh_best)
        summed = summed * shrink + jnp.sum(weights, axis=-1)
        accum = accum * shrink[..., None] + jnp.einsum(
            "kgtn,nkd->kgtd",
            weights.astype(jnp.bfloat16),
            value_rows,
            preferred_element_type=jnp.float32,
        )
        return (fresh_best, summed, accum)

    def absorb(running, stacked, offset):
        amount = stacked.shape[1]
        needed = (offset + amount > lowest) & (offset <= highest)
        return lax.cond(
            needed, lambda inner: update(inner, stacked, offset), lambda inner: inner, running
        )

    start_state = (
        jnp.full((kv_local, group_size, tokens_here), -1e30, jnp.float32),
        jnp.zeros((kv_local, group_size, tokens_here), jnp.float32),
        jnp.zeros((kv_local, group_size, tokens_here, HEAD_DIM), jnp.float32),
    )
    paired = jnp.concatenate([keys, values], axis=0)
    reach = lax.axis_size("row") // 2 + 1
    running = absorb(start_state, paired, first_pos)

    def advance(step_id, loop_state):
        inner, moving = loop_state
        moving = from_behind(moving, "row", 1)
        return (absorb(inner, moving, (row_pos - step_id) * tokens_here), moving)

    running, _ = lax.fori_loop(1, reach + 1, advance, (running, paired))
    _, summed, accum = running
    mixed = accum / summed[..., None]
    outputs = (
        jnp.transpose(mixed, (2, 0, 1, 3))
        .reshape(tokens_here, heads_local * HEAD_DIM)
        .astype(jnp.bfloat16)[None]
    )
    half_heads = heads_local // 2
    partner = swapped(outputs, "mp", 0)
    model_pos = lax.axis_index("mp")
    is_policy = model_pos == 0
    policy = jnp.where(is_policy, outputs[0], partner[0])
    anchor = jnp.where(is_policy, partner[0], outputs[0])
    column_at = model_pos * half_heads * HEAD_DIM
    policy_part = lax.dynamic_slice_in_dim(policy, column_at, half_heads * HEAD_DIM, 1)
    anchor_part = lax.dynamic_slice_in_dim(anchor, column_at, half_heads * HEAD_DIM, 1)
    gap = relative_gap(policy_part, anchor_part, tokens_here, half_heads)
    return (outputs, gap)


SCALE = math.log2(math.e) / math.sqrt(HEAD_DIM)
GROUP = HEADS // KV_HEADS
BIG = 2.0**100
LIMIT = 2.0**100
PIECES = 4
NT = (((1,), (1,)), ((), ()))
VMEM = pl.BlockSpec(memory_space=pltpu.VMEM)
SMEM = pl.BlockSpec(memory_space=pltpu.SMEM)
HBM = pl.BlockSpec(memory_space=pltpu.HBM)


def lanes(index, width):
    if isinstance(index, int):
        return pl.ds(index * width, width)
    return pl.ds(pl.multiple_of(index * width, width), width)


def with_ones(value_rows):
    return jnp.concatenate([value_rows, jnp.ones_like(value_rows)], axis=1)


def scores_of(query_rows, key_rows):
    return lax.dot_general(query_rows, key_rows, NT, preferred_element_type=jnp.float32)


def mass_of(scores):
    return jnp.exp2(scores * SCALE).astype(jnp.bfloat16)


def spread(mass, value_rows):
    return jnp.dot(mass, value_rows, preferred_element_type=jnp.float32)


def in_columns(shape, *columns):
    lane = lax.broadcasted_iota(jnp.int32, shape, 1)
    tile = jnp.zeros(shape, jnp.float32)
    for index, column in enumerate(columns):
        tile = jnp.where(lane == index, column, tile)
    return tile


def column_copies(source, target, sems, pieces):
    rows = target.shape[0] // pieces
    return [
        pltpu.make_async_copy(
            source.at[pl.ds(piece * rows, rows)], target.at[pl.ds(piece * rows, rows)], sems[piece]
        )
        for piece in range(pieces)
    ]


def run_all(copies):
    for copy in copies:
        copy.start()
    for copy in copies:
        copy.wait()


def pack_copies(which, k_hbm, v_hbm, pack_ref, sem):
    width = pack_ref.shape[2]
    copies = []
    for index, ref in enumerate((k_hbm, v_hbm)):
        sems = [sem.at[index * PIECES + piece] for piece in range(PIECES)]
        copies += column_copies(ref.at[0, :, lanes(which, width)], pack_ref.at[index], sems, PIECES)
    return copies


def pack_kernel(k_hbm, v_hbm, pack_ref, sem):
    run_all(pack_copies(1 - lax.axis_index("mp"), k_hbm, v_hbm, pack_ref, sem))


def load_kernel(k_hbm, v_hbm, q_hbm, after_ref, pack_ref, q_ref, sem):
    del after_ref
    mp = lax.axis_index("mp")
    width = q_ref.shape[1] // 2
    copies = pack_copies(mp, k_hbm, v_hbm, pack_ref, sem)
    for index, which in enumerate((1 - mp, mp)):
        copies += column_copies(
            q_hbm.at[0, :, lanes(which, width)],
            q_ref.at[:, lanes(index, width)],
            [sem.at[2 * PIECES + index]],
            1,
        )
    run_all(copies)


def diagonal_kernel(
    len_hbm, q_ref, other_ref, own_ref, wide_ref, acc_ref, near_ref, far_ref, bias_ref, len_ref, sem
):
    tokens_here = q_ref.shape[0]
    half = tokens_here // 2
    row_pos = lax.axis_index("row")
    kv_half = other_ref.shape[2] // HEAD_DIM
    len_copy = pltpu.make_async_copy(len_hbm, len_ref, sem.at[0])
    len_copy.start()
    len_copy.wait()
    boundary = len_ref[0] - row_pos * tokens_here
    query = lax.broadcasted_iota(jnp.int32, (tokens_here, tokens_here), 0)
    key = lax.broadcasted_iota(jnp.int32, (tokens_here, tokens_here), 1)
    kept = (key <= query) & ((query < boundary) | (key >= boundary))
    bias_ref[...] = jnp.where(kept, 0.0, -jnp.inf)
    tile = (tokens_here, HEAD_DIM)
    token = lax.broadcasted_iota(jnp.int32, tile, 0)
    for hops, ref in ((1, near_ref), (2, far_ref)):
        gone = jnp.where(row_pos >= hops, 0.0, -BIG)
        before = jnp.where(token - hops * tokens_here < boundary, -BIG, 0.0)
        ref[...] = in_columns(tile, -1.0, before, gone).astype(jnp.bfloat16)
    later = in_columns(tile, 0.0, jnp.where(token >= boundary, 1.0, 0.0), 1.0)
    first_lane = lax.broadcasted_iota(jnp.int32, (half, HEAD_DIM), 1) == 0
    for step in range(2 * kv_half):
        pack_ref = other_ref if step < kv_half else own_ref
        key_rows = pack_ref[0, :, lanes(step % kv_half, HEAD_DIM)]
        value_rows = value_of(pack_ref, step % kv_half)
        for g in range(GROUP):
            local = step * GROUP + g
            for low in (0, half):
                rows = pl.ds(low, half)
                seen = low + half
                query_rows = q_ref[rows, lanes(local, HEAD_DIM)]
                scores = scores_of(query_rows, key_rows[:seen]) + bias_ref[rows, :seen]
                top = jnp.max(scores, axis=1, keepdims=True).astype(jnp.bfloat16)
                top = top.astype(jnp.float32)
                acc_ref[rows, lanes(local, 2 * HEAD_DIM)] = spread(
                    mass_of(scores - top), value_rows[:seen]
                )
                extra = jnp.where(first_lane, top, later[low:seen]).astype(jnp.bfloat16)
                wide_ref[rows, lanes(2 * local, HEAD_DIM)] = query_rows
                wide_ref[rows, lanes(2 * local + 1, HEAD_DIM)] = extra


def key_of(kv_ref, kv, tile_ref):
    return jnp.concatenate([kv_ref[0, :, lanes(kv, HEAD_DIM)], tile_ref[...]], axis=1)


def value_of(kv_ref, kv):
    return with_ones(kv_ref[1, :, lanes(kv, HEAD_DIM)])


def near_kernel(own, wide_ref, kv_ref, acc_in, tile_ref, acc_ref):
    heads_half = acc_ref.shape[1] // (2 * HEAD_DIM)
    first_head = heads_half if own else 0
    for local in range(heads_half):
        if local % GROUP == 0:
            key_rows = key_of(kv_ref, local // GROUP, tile_ref)
            value_rows = value_of(kv_ref, local // GROUP)
        cols = lanes(first_head + local, 2 * HEAD_DIM)
        mass = mass_of(scores_of(wide_ref[:, cols], key_rows))
        acc_ref[:, lanes(local, 2 * HEAD_DIM)] = acc_in[:, cols] + spread(mass, value_rows)


def far_heads(first_head, refs, store):
    wide_ref, _, far_kv, _, acc_ref, _, far_tile = refs
    worst = None
    for local in range(acc_ref.shape[1] // (2 * HEAD_DIM)):
        if local % GROUP == 0:
            key_rows = key_of(far_kv, local // GROUP, far_tile)
            value_rows = value_of(far_kv, local // GROUP)
        mass = mass_of(scores_of(wide_ref[:, lanes(first_head + local, 2 * HEAD_DIM)], key_rows))
        acc = acc_ref[:, lanes(local, 2 * HEAD_DIM)] + spread(mass, value_rows)
        total = acc[:, HEAD_DIM:]
        store(local, (acc[:, :HEAD_DIM] / total).astype(jnp.bfloat16))
        worst = total if worst is None else jnp.maximum(worst, total)
    return jnp.logical_not(jnp.max(worst) < LIMIT)


def far_heads_again(first_head, refs, store):
    wide_ref, near_kv, far_kv, first_ref, acc_ref, near_tile, far_tile = refs

    @pl.loop(0, acc_ref.shape[1] // (2 * HEAD_DIM))
    def _(local):
        cols = lanes(first_head + local, 2 * HEAD_DIM)
        query_rows = wide_ref[:, cols]
        kv = local // GROUP
        near_scores = scores_of(query_rows, key_of(near_kv, kv, near_tile))
        far_scores = scores_of(query_rows, key_of(far_kv, kv, far_tile))
        top = jnp.max(jnp.maximum(near_scores, far_scores), axis=1, keepdims=True)
        top = jnp.maximum(top, 0.0)
        acc = (
            first_ref[:, cols] * jnp.exp2(-top * SCALE)
            + spread(mass_of(near_scores - top), value_of(near_kv, kv))
            + spread(mass_of(far_scores - top), value_of(far_kv, kv))
        )
        store(local, (acc[:, :HEAD_DIM] / acc[:, HEAD_DIM:]).astype(jnp.bfloat16))


def far_other_kernel(*refs):
    refs, out_ref = refs[:7], refs[7]
    first_head = 0

    def store(local, block):
        out_ref[0, :, lanes(local, HEAD_DIM)] = block

    too_high = far_heads(first_head, refs, store)

    @pl.when(too_high)
    def _():
        far_heads_again(first_head, refs, store)


def far_own_kernel(*refs):
    refs, (sent_ref, got_ref, out_ref, gap_out, mine_ref, gap_ref, sem) = refs[:7], refs[7:]
    width = sent_ref.shape[2]
    tokens_here = sent_ref.shape[1]
    heads_half = width // HEAD_DIM
    mp = lax.axis_index("mp")
    first_head = heads_half
    sent_copy = pltpu.make_async_copy(
        sent_ref.at[0], out_ref.at[0, :, lanes(1 - mp, width)], sem.at[heads_half]
    )
    sent_copy.start()
    gap_copy = pltpu.make_async_copy(gap_ref, gap_out, sem.at[heads_half + 1])

    def mine_copy(local):
        return pltpu.make_async_copy(
            mine_ref.at[:, lanes(local, HEAD_DIM)],
            out_ref.at[0, :, lanes(mp * heads_half + local, HEAD_DIM)],
            sem.at[local],
        )

    lane = lax.broadcasted_iota(jnp.int32, (tokens_here, HEAD_DIM), 1)
    state = {"far": jnp.zeros((tokens_here, HEAD_DIM), jnp.float32)}
    state["size"] = state["far"]

    def squares(local, block):
        mine = block.astype(jnp.float32)
        theirs = got_ref[0, :, lanes(local, HEAD_DIM)].astype(jnp.float32)
        difference = mine - theirs
        policy = jnp.where(mp == 0, mine, theirs)
        return (
            jnp.sum(difference * difference, axis=1, keepdims=True),
            jnp.sum(policy * policy, axis=1, keepdims=True),
        )

    def gap_of(far, size):
        return far.T[:heads_half] / HEAD_DIM / (size.T[:heads_half] / HEAD_DIM + 1e-06)

    def store(local, block):
        mine_ref[:, lanes(local, HEAD_DIM)] = block
        mine_copy(local).start()
        far, size = squares(local, block)
        state["far"] = jnp.where(lane == local, far, state["far"])
        state["size"] = jnp.where(lane == local, size, state["size"])

    too_high = far_heads(first_head, refs, store)
    gap_ref[...] = gap_of(state["far"], state["size"])
    gap_copy.start()
    sent_copy.wait()
    for local in range(heads_half):
        mine_copy(local).wait()
    gap_copy.wait()

    @pl.when(too_high)
    def _():
        def store_again(local, block):
            mine_ref[:, lanes(local, HEAD_DIM)] = block

        far_heads_again(first_head, refs, store_again)
        far = size = jnp.zeros((tokens_here, HEAD_DIM), jnp.float32)
        for local in range(heads_half):
            parts = squares(local, mine_ref[:, lanes(local, HEAD_DIM)])
            far = jnp.where(lane == local, parts[0], far)
            size = jnp.where(lane == local, parts[1], size)
            mine_copy(local).start()
        gap_ref[...] = gap_of(far, size)
        gap_copy.start()
        for local in range(heads_half):
            mine_copy(local).wait()
        gap_copy.wait()


def in_hbm(array):
    return pltpu.with_memory_space_constraint(array, pltpu.HBM)


def call(kernel, out_shape, in_specs, out_specs, flops, vmem_mib=16, **more):
    return pl.pallas_call(
        kernel,
        out_shape=out_shape,
        in_specs=in_specs,
        out_specs=out_specs,
        cost_estimate=pl.CostEstimate(
            flops=int(flops), bytes_accessed=4 << 20, transcendentals=0
        ),
        compiler_params=pltpu.CompilerParams(vmem_limit_bytes=vmem_mib * 2**20),
        **more,
    )


def per_device_paired(queries, keys, values, lengths):
    tokens_here = queries.shape[1]
    kv_local = keys.shape[2] // HEAD_DIM
    heads_local = kv_local * GROUP
    width = heads_local * HEAD_DIM
    half = width // 2
    half_kv = keys.shape[2] // 2
    count = lax.axis_size("row")
    f32, bf16 = jnp.float32, jnp.bfloat16
    shape = jax.ShapeDtypeStruct
    tile_type = shape((tokens_here, HEAD_DIM), bf16)
    work = 8 * heads_local * tokens_here * tokens_here * HEAD_DIM

    near_route = [(i - 1, i) for i in range(1, count)]
    far_route = [(i - 1, i) for i in range(2, count)]
    pack_type = shape((2, tokens_here, half_kv), bf16)
    other = call(
        pack_kernel,
        pack_type,
        [HBM] * 2,
        VMEM,
        work,
        scratch_shapes=[pltpu.SemaphoreType.DMA((2 * PIECES,))],
    )(in_hbm(keys), in_hbm(values))
    other_near = lax.ppermute(other, "row", near_route)
    own, query_rows = call(
        load_kernel,
        (pack_type, shape((tokens_here, width), bf16)),
        [HBM] * 4,
        [VMEM] * 2,
        work,
        scratch_shapes=[pltpu.SemaphoreType.DMA((2 * PIECES + 2,))],
    )(in_hbm(keys), in_hbm(values), in_hbm(queries), other)
    own_near = lax.ppermute(own, "row", near_route)
    wide, acc, near_tile, far_tile = call(
        diagonal_kernel,
        (
            shape((tokens_here, 2 * width), bf16),
            shape((tokens_here, 2 * width), f32),
            tile_type,
            tile_type,
        ),
        [HBM] + [VMEM] * 3,
        [VMEM] * 4,
        work,
        vmem_mib=16,
        scratch_shapes=[
            pltpu.VMEM((tokens_here, tokens_here), f32),
            pltpu.SMEM(lengths.shape, jnp.int32),
            pltpu.SemaphoreType.DMA((1,)),
        ],
    )(in_hbm(lengths), query_rows, other, own)
    other_far = lax.ppermute(other_near, "row", far_route)

    def near(own, block):
        return call(
            lambda *refs: near_kernel(own, *refs),
            shape((tokens_here, width), f32),
            [VMEM] * 4,
            VMEM,
            work,
        )(wide, block, acc, near_tile)

    other_acc = near(False, other_near)
    own_far = lax.ppermute(own_near, "row", far_route)
    own_acc = near(True, own_near)
    sent = call(
        far_other_kernel, shape((1, tokens_here, half), bf16), [VMEM] * 7, VMEM, work
    )(wide, other_near, other_far, acc, other_acc, near_tile, far_tile)
    got = lax.ppermute(sent, "mp", [(0, 1), (1, 0)])
    outputs, gap = call(
        far_own_kernel,
        (
            shape((1, tokens_here, width), bf16),
            shape((heads_local // 2, tokens_here), f32),
        ),
        [VMEM] * 9,
        [HBM, HBM],
        work,
        scratch_shapes=[
            pltpu.VMEM((tokens_here, half), bf16),
            pltpu.VMEM((heads_local // 2, tokens_here), f32),
            pltpu.SemaphoreType.DMA((2 + heads_local // 2,)),
        ],
    )(wide, own_near, own_far, acc, own_acc, near_tile, far_tile, sent, got)
    return (outputs, gap)


def two_hops(mesh, rollouts):
    return rollouts == 2 and mesh.shape["row"] // 2 == 2 and mesh.shape["mp"] == 2


def solution(mesh):
    in_specs = (
        P("mp", ("groups", "row"), "col"),
        P("mp", ("groups", "row"), "col"),
        P("mp", ("groups", "row"), "col"),
        P("groups"),
    )
    out_specs = (P("mp", ("groups", "row"), "col"), P(("col", "mp"), ("groups", "row")))

    def place(body):
        return jax.shard_map(
            body, mesh=mesh, in_specs=in_specs, out_specs=out_specs, check_vma=False
        )

    def step(queries, keys, values, lengths):
        rollouts = lengths.shape[0] // mesh.shape["groups"]
        kv_local = keys.shape[2] // HEAD_DIM // mesh.shape["col"]
        if not two_hops(mesh, rollouts) or kv_local % 2:
            return place(per_device_general)(queries, keys, values, lengths)
        return place(per_device_paired)(queries, keys, values, lengths)

    return step
```

```python
import math

import jax
import jax.numpy as jnp
from jax import lax
from jax.experimental import pallas as pl
from jax.experimental.pallas import tpu as pltpu
from jax.sharding import PartitionSpec as P

HEADS = 40
KV_HEADS = 8
HEAD_DIM = 128


def from_behind(block, axis, distance):
    devices = range(lax.axis_size(axis))
    route = [(i - distance, i) for i in devices if i - distance in devices]
    return lax.ppermute(block, axis, route)


def swapped(block, axis, distance):
    count = lax.axis_size(axis)
    route = []
    for low in range(count):
        high = low | 1 << distance
        if high != low and high < count:
            route += [(low, high), (high, low)]
    return lax.ppermute(block, axis, route)


def relative_gap(first, second, tokens_here, heads_count):
    first = first.astype(jnp.float32).reshape(tokens_here, heads_count, HEAD_DIM)
    second = second.astype(jnp.float32).reshape(tokens_here, heads_count, HEAD_DIM)
    difference = first - second
    scale_sum = jnp.mean(first * first, axis=-1) + 1e-06
    return jnp.transpose(jnp.mean(difference * difference, axis=-1) / scale_sum)


def per_device_general(queries, keys, values, lengths):
    tokens_here = queries.shape[1]
    width_here = keys.shape[2]
    kv_local = width_here // HEAD_DIM
    group_size = HEADS // KV_HEADS
    heads_local = kv_local * group_size
    factor = 1.0 / math.sqrt(HEAD_DIM)
    row_pos = lax.axis_index("row")
    first_pos = row_pos * tokens_here
    query_pos = first_pos + jnp.arange(tokens_here, dtype=jnp.int32)
    finish = jnp.cumsum(lengths)
    begin_at = jnp.sum(
        jnp.where(finish[None, :] <= query_pos[:, None], lengths[None, :], 0), axis=1
    )
    lowest = begin_at[0]
    highest = first_pos + tokens_here - 1
    query_rows = queries[0].reshape(tokens_here, kv_local, group_size, HEAD_DIM)

    def update(running, stacked, offset):
        best, summed, accum = running
        amount = stacked.shape[1]
        key_rows = stacked[0].reshape(amount, kv_local, HEAD_DIM)
        value_rows = stacked[1].reshape(amount, kv_local, HEAD_DIM)
        scores = (
            jnp.einsum("tkgd,nkd->kgtn", query_rows, key_rows, preferred_element_type=jnp.float32)
            * factor
        )
        key_pos = offset + jnp.arange(amount, dtype=jnp.int32)
        allowed = (key_pos[None, :] >= begin_at[:, None]) & (key_pos[None, :] <= query_pos[:, None])
        masked = jnp.where(allowed, scores, -jnp.inf)
        fresh_best = jnp.maximum(best, jnp.max(masked, axis=-1))
        weights = jnp.where(allowed, jnp.exp(masked - fresh_best[..., None]), 0.0)
        shrink = jnp.exp(best - fresh_best)
        summed = summed * shrink + jnp.sum(weights, axis=-1)
        accum = accum * shrink[..., None] + jnp.einsum(
            "kgtn,nkd->kgtd",
            weights.astype(jnp.bfloat16),
            value_rows,
            preferred_element_type=jnp.float32,
        )
        return (fresh_best, summed, accum)

    def absorb(running, stacked, offset):
        amount = stacked.shape[1]
        needed = (offset + amount > lowest) & (offset <= highest)
        return lax.cond(
            needed, lambda inner: update(inner, stacked, offset), lambda inner: inner, running
        )

    start_state = (
        jnp.full((kv_local, group_size, tokens_here), -1e30, jnp.float32),
        jnp.zeros((kv_local, group_size, tokens_here), jnp.float32),
        jnp.zeros((kv_local, group_size, tokens_here, HEAD_DIM), jnp.float32),
    )
    paired = jnp.concatenate([keys, values], axis=0)
    reach = lax.axis_size("row") // 2 + 1
    running = absorb(start_state, paired, first_pos)

    def advance(step_id, loop_state):
        inner, moving = loop_state
        moving = from_behind(moving, "row", 1)
        return (absorb(inner, moving, (row_pos - step_id) * tokens_here), moving)

    running, _ = lax.fori_loop(1, reach + 1, advance, (running, paired))
    _, summed, accum = running
    mixed = accum / summed[..., None]
    outputs = (
        jnp.transpose(mixed, (2, 0, 1, 3))
        .reshape(tokens_here, heads_local * HEAD_DIM)
        .astype(jnp.bfloat16)[None]
    )
    half_heads = heads_local // 2
    partner = swapped(outputs, "mp", 0)
    model_pos = lax.axis_index("mp")
    is_policy = model_pos == 0
    policy = jnp.where(is_policy, outputs[0], partner[0])
    anchor = jnp.where(is_policy, partner[0], outputs[0])
    column_at = model_pos * half_heads * HEAD_DIM
    policy_part = lax.dynamic_slice_in_dim(policy, column_at, half_heads * HEAD_DIM, 1)
    anchor_part = lax.dynamic_slice_in_dim(anchor, column_at, half_heads * HEAD_DIM, 1)
    gap = relative_gap(policy_part, anchor_part, tokens_here, half_heads)
    return (outputs, gap)


SCALE = math.log2(math.e) / math.sqrt(HEAD_DIM)
GROUP = HEADS // KV_HEADS
BIG = 2.0**100
LIMIT = 2.0**100
PIECES = 4
NT = (((1,), (1,)), ((), ()))
VMEM = pl.BlockSpec(memory_space=pltpu.VMEM)
SMEM = pl.BlockSpec(memory_space=pltpu.SMEM)
HBM = pl.BlockSpec(memory_space=pltpu.HBM)


def lanes(index, width):
    if isinstance(index, int):
        return pl.ds(index * width, width)
    return pl.ds(pl.multiple_of(index * width, width), width)


def with_ones(value_rows):
    return jnp.concatenate([value_rows, jnp.ones_like(value_rows)], axis=1)


def scores_of(query_rows, key_rows):
    return lax.dot_general(query_rows, key_rows, NT, preferred_element_type=jnp.float32)


def mass_of(scores):
    return jnp.exp2(scores * SCALE).astype(jnp.bfloat16)


def product(left, right):
    return jnp.dot(left, right, preferred_element_type=jnp.float32)


def in_columns(shape, *columns):
    lane = lax.broadcasted_iota(jnp.int32, shape, 1)
    tile = jnp.zeros(shape, jnp.float32)
    for index, column in enumerate(columns):
        tile = jnp.where(lane == index, column, tile)
    return tile


def column_copies(source, target, sems, pieces):
    rows = target.shape[0] // pieces
    return [
        pltpu.make_async_copy(
            source.at[pl.ds(piece * rows, rows)], target.at[pl.ds(piece * rows, rows)], sems[piece]
        )
        for piece in range(pieces)
    ]


def run_all(copies):
    for copy in copies:
        copy.start()
    for copy in copies:
        copy.wait()


def pack_copies(which, k_hbm, v_hbm, pack_ref, sem):
    width = pack_ref.shape[2]
    copies = []
    for index, ref in enumerate((k_hbm, v_hbm)):
        sems = [sem.at[index * PIECES + piece] for piece in range(PIECES)]
        copies += column_copies(ref.at[0, :, lanes(which, width)], pack_ref.at[index], sems, PIECES)
    return copies


def pack_kernel(k_hbm, v_hbm, pack_ref, sem):
    run_all(pack_copies(1 - lax.axis_index("mp"), k_hbm, v_hbm, pack_ref, sem))


def load_kernel(k_hbm, v_hbm, q_hbm, after_ref, pack_ref, q_ref, sem):
    del after_ref
    mp = lax.axis_index("mp")
    width = q_ref.shape[1] // 2
    copies = pack_copies(mp, k_hbm, v_hbm, pack_ref, sem)
    for index, which in enumerate((1 - mp, mp)):
        copies += column_copies(
            q_hbm.at[0, :, lanes(which, width)],
            q_ref.at[:, lanes(index, width)],
            [sem.at[2 * PIECES + index]],
            1,
        )
    run_all(copies)


def diagonal_kernel(
    len_hbm, q_ref, other_ref, own_ref, wide_ref, acc_ref, near_ref, far_ref, bias_ref, len_ref, sem
):
    tokens_here = q_ref.shape[0]
    half = tokens_here // 2
    row_pos = lax.axis_index("row")
    kv_half = other_ref.shape[2] // HEAD_DIM
    len_copy = pltpu.make_async_copy(len_hbm, len_ref, sem.at[0])
    len_copy.start()
    len_copy.wait()
    boundary = len_ref[0] - row_pos * tokens_here
    query = lax.broadcasted_iota(jnp.int32, (tokens_here, tokens_here), 0)
    key = lax.broadcasted_iota(jnp.int32, (tokens_here, tokens_here), 1)
    kept = (key <= query) & ((query < boundary) | (key >= boundary))
    bias_ref[...] = jnp.where(kept, 0.0, -jnp.inf)
    tile = (tokens_here, HEAD_DIM)
    token = lax.broadcasted_iota(jnp.int32, tile, 0)
    for hops, ref in ((1, near_ref), (2, far_ref)):
        gone = jnp.where(row_pos >= hops, 0.0, -BIG)
        before = jnp.where(token - hops * tokens_here < boundary, -BIG, 0.0)
        ref[...] = in_columns(tile, -1.0, before, gone).T.astype(jnp.bfloat16)
    later = in_columns(tile, 0.0, jnp.where(token >= boundary, 1.0, 0.0), 1.0)
    first_lane = lax.broadcasted_iota(jnp.int32, (half, HEAD_DIM), 1) == 0
    for step in range(2 * kv_half):
        pack_ref = other_ref if step < kv_half else own_ref
        key_rows = pack_ref[0, :, lanes(step % kv_half, HEAD_DIM)]
        value_rows = value_of(pack_ref, step % kv_half)
        for g in range(GROUP):
            local = step * GROUP + g
            for low in (0, half):
                rows = pl.ds(low, half)
                seen = low + half
                query_rows = q_ref[rows, lanes(local, HEAD_DIM)]
                scores = scores_of(query_rows, key_rows[:seen]) + bias_ref[rows, :seen]
                top = jnp.max(scores, axis=1, keepdims=True).astype(jnp.bfloat16)
                top = top.astype(jnp.float32)
                spot = pl.ds(local * tokens_here + low, half)
                acc_ref[spot, :] = product(mass_of(scores - top), value_rows[:seen])
                extra = jnp.where(first_lane, top, later[low:seen]).astype(jnp.bfloat16)
                wide_ref[spot, :] = jnp.concatenate([query_rows, extra], axis=1)


def key_of(kv_ref, kv, tile_ref):
    return jnp.concatenate([kv_ref[0, :, lanes(kv, HEAD_DIM)].T, tile_ref[...]], axis=0)


def value_of(kv_ref, kv):
    return with_ones(kv_ref[1, :, lanes(kv, HEAD_DIM)])


def group_rows(tokens_here, group):
    return pl.ds(group * GROUP * tokens_here, GROUP * tokens_here)


def near_kernel(own, wide_ref, kv_ref, acc_in, tile_ref, acc_ref):
    tokens_here = tile_ref.shape[1]
    kv_half = acc_ref.shape[0] // (GROUP * tokens_here)
    for kv in range(kv_half):
        rows = group_rows(tokens_here, kv + (kv_half if own else 0))
        mass = mass_of(product(wide_ref[rows, :], key_of(kv_ref, kv, tile_ref)))
        acc_ref[group_rows(tokens_here, kv), :] = acc_in[rows, :] + product(
            mass, value_of(kv_ref, kv)
        )


def far_heads(first_group, refs, store):
    wide_ref, _, far_kv, _, acc_ref, _, far_tile = refs
    tokens_here = far_tile.shape[1]
    worst = None
    for kv in range(acc_ref.shape[0] // (GROUP * tokens_here)):
        rows = group_rows(tokens_here, first_group + kv)
        mass = mass_of(product(wide_ref[rows, :], key_of(far_kv, kv, far_tile)))
        acc = acc_ref[group_rows(tokens_here, kv), :] + product(mass, value_of(far_kv, kv))
        for g in range(GROUP):
            part = acc[g * tokens_here : (g + 1) * tokens_here]
            total = part[:, HEAD_DIM:]
            store(kv * GROUP + g, (part[:, :HEAD_DIM] / total).astype(jnp.bfloat16))
            worst = total if worst is None else jnp.maximum(worst, total)
    return jnp.logical_not(jnp.max(worst) < LIMIT)


def far_heads_again(first_group, refs, store):
    wide_ref, near_kv, far_kv, first_ref, acc_ref, near_tile, far_tile = refs
    tokens_here = far_tile.shape[1]

    @pl.loop(0, acc_ref.shape[0] // tokens_here)
    def _(local):
        head = first_group * GROUP + local
        rows = pl.ds(pl.multiple_of(head * tokens_here, tokens_here), tokens_here)
        query_rows = wide_ref[rows, :]
        kv = local // GROUP
        near_scores = product(query_rows, key_of(near_kv, kv, near_tile))
        far_scores = product(query_rows, key_of(far_kv, kv, far_tile))
        top = jnp.max(jnp.maximum(near_scores, far_scores), axis=1, keepdims=True)
        top = jnp.maximum(top, 0.0)
        acc = (
            first_ref[rows, :] * jnp.exp2(-top * SCALE)
            + product(mass_of(near_scores - top), value_of(near_kv, kv))
            + product(mass_of(far_scores - top), value_of(far_kv, kv))
        )
        store(local, (acc[:, :HEAD_DIM] / acc[:, HEAD_DIM:]).astype(jnp.bfloat16))


def far_other_kernel(*refs):
    refs, out_ref = refs[:7], refs[7]

    def store(local, block):
        out_ref[0, :, lanes(local, HEAD_DIM)] = block

    too_high = far_heads(0, refs, store)

    @pl.when(too_high)
    def _():
        far_heads_again(0, refs, store)


def far_own_kernel(*refs):
    refs, (sent_ref, got_ref, out_ref, gap_out, mine_ref, gap_ref, sem) = refs[:7], refs[7:]
    width = sent_ref.shape[2]
    tokens_here = sent_ref.shape[1]
    heads_half = width // HEAD_DIM
    mp = lax.axis_index("mp")
    first_group = heads_half // GROUP
    sent_copy = pltpu.make_async_copy(
        sent_ref.at[0], out_ref.at[0, :, lanes(1 - mp, width)], sem.at[heads_half]
    )
    sent_copy.start()
    gap_copy = pltpu.make_async_copy(gap_ref, gap_out, sem.at[heads_half + 1])

    def mine_copy(local):
        return pltpu.make_async_copy(
            mine_ref.at[:, lanes(local, HEAD_DIM)],
            out_ref.at[0, :, lanes(mp * heads_half + local, HEAD_DIM)],
            sem.at[local],
        )

    lane = lax.broadcasted_iota(jnp.int32, (tokens_here, HEAD_DIM), 1)
    state = {"far": jnp.zeros((tokens_here, HEAD_DIM), jnp.float32)}
    state["size"] = state["far"]

    def squares(local, block):
        mine = block.astype(jnp.float32)
        theirs = got_ref[0, :, lanes(local, HEAD_DIM)].astype(jnp.float32)
        difference = mine - theirs
        policy = jnp.where(mp == 0, mine, theirs)
        return (
            jnp.sum(difference * difference, axis=1, keepdims=True),
            jnp.sum(policy * policy, axis=1, keepdims=True),
        )

    def gap_of(far, size):
        return far.T[:heads_half] / HEAD_DIM / (size.T[:heads_half] / HEAD_DIM + 1e-06)

    def store(local, block):
        mine_ref[:, lanes(local, HEAD_DIM)] = block
        mine_copy(local).start()
        far, size = squares(local, block)
        state["far"] = jnp.where(lane == local, far, state["far"])
        state["size"] = jnp.where(lane == local, size, state["size"])

    too_high = far_heads(first_group, refs, store)
    gap_ref[...] = gap_of(state["far"], state["size"])
    gap_copy.start()
    sent_copy.wait()
    for local in range(heads_half):
        mine_copy(local).wait()
    gap_copy.wait()

    @pl.when(too_high)
    def _():
        def store_again(local, block):
            mine_ref[:, lanes(local, HEAD_DIM)] = block

        far_heads_again(first_group, refs, store_again)
        far = size = jnp.zeros((tokens_here, HEAD_DIM), jnp.float32)
        for local in range(heads_half):
            parts = squares(local, mine_ref[:, lanes(local, HEAD_DIM)])
            far = jnp.where(lane == local, parts[0], far)
            size = jnp.where(lane == local, parts[1], size)
            mine_copy(local).start()
        gap_ref[...] = gap_of(far, size)
        gap_copy.start()
        for local in range(heads_half):
            mine_copy(local).wait()
        gap_copy.wait()


def in_hbm(array):
    return pltpu.with_memory_space_constraint(array, pltpu.HBM)


def call(kernel, out_shape, in_specs, out_specs, flops, vmem_mib=16, **more):
    return pl.pallas_call(
        kernel,
        out_shape=out_shape,
        in_specs=in_specs,
        out_specs=out_specs,
        cost_estimate=pl.CostEstimate(
            flops=int(flops), bytes_accessed=4 << 20, transcendentals=0
        ),
        compiler_params=pltpu.CompilerParams(vmem_limit_bytes=vmem_mib * 2**20),
        **more,
    )


def per_device_paired(queries, keys, values, lengths):
    tokens_here = queries.shape[1]
    kv_local = keys.shape[2] // HEAD_DIM
    heads_local = kv_local * GROUP
    width = heads_local * HEAD_DIM
    half = width // 2
    half_kv = keys.shape[2] // 2
    count = lax.axis_size("row")
    f32, bf16 = jnp.float32, jnp.bfloat16
    shape = jax.ShapeDtypeStruct
    tile_type = shape((HEAD_DIM, tokens_here), bf16)
    work = 8 * heads_local * tokens_here * tokens_here * HEAD_DIM

    near_route = [(i - 1, i) for i in range(1, count)]
    far_route = [(i - 1, i) for i in range(2, count)]
    pack_type = shape((2, tokens_here, half_kv), bf16)
    other = call(
        pack_kernel,
        pack_type,
        [HBM] * 2,
        VMEM,
        work,
        scratch_shapes=[pltpu.SemaphoreType.DMA((2 * PIECES,))],
    )(in_hbm(keys), in_hbm(values))
    other_near = lax.ppermute(other, "row", near_route)
    own, query_rows = call(
        load_kernel,
        (pack_type, shape((tokens_here, width), bf16)),
        [HBM] * 4,
        [VMEM] * 2,
        work,
        scratch_shapes=[pltpu.SemaphoreType.DMA((2 * PIECES + 2,))],
    )(in_hbm(keys), in_hbm(values), in_hbm(queries), other)
    own_near = lax.ppermute(own, "row", near_route)
    wide, acc, near_tile, far_tile = call(
        diagonal_kernel,
        (
            shape((heads_local * tokens_here, 2 * HEAD_DIM), bf16),
            shape((heads_local * tokens_here, 2 * HEAD_DIM), f32),
            tile_type,
            tile_type,
        ),
        [HBM] + [VMEM] * 3,
        [VMEM] * 4,
        work,
        vmem_mib=16,
        scratch_shapes=[
            pltpu.VMEM((tokens_here, tokens_here), f32),
            pltpu.SMEM(lengths.shape, jnp.int32),
            pltpu.SemaphoreType.DMA((1,)),
        ],
    )(in_hbm(lengths), query_rows, other, own)
    other_far = lax.ppermute(other_near, "row", far_route)

    def near(own, block):
        return call(
            lambda *refs: near_kernel(own, *refs),
            shape((heads_local // 2 * tokens_here, 2 * HEAD_DIM), f32),
            [VMEM] * 4,
            VMEM,
            work,
        )(wide, block, acc, near_tile)

    other_acc = near(False, other_near)
    own_far = lax.ppermute(own_near, "row", far_route)
    own_acc = near(True, own_near)
    sent = call(
        far_other_kernel, shape((1, tokens_here, half), bf16), [VMEM] * 7, VMEM, work
    )(wide, other_near, other_far, acc, other_acc, near_tile, far_tile)
    got = lax.ppermute(sent, "mp", [(0, 1), (1, 0)])
    outputs, gap = call(
        far_own_kernel,
        (
            shape((1, tokens_here, width), bf16),
            shape((heads_local // 2, tokens_here), f32),
        ),
        [VMEM] * 9,
        [HBM, HBM],
        work,
        scratch_shapes=[
            pltpu.VMEM((tokens_here, half), bf16),
            pltpu.VMEM((heads_local // 2, tokens_here), f32),
            pltpu.SemaphoreType.DMA((2 + heads_local // 2,)),
        ],
    )(wide, own_near, own_far, acc, own_acc, near_tile, far_tile, sent, got)
    return (outputs, gap)


def two_hops(mesh, rollouts):
    return rollouts == 2 and mesh.shape["row"] // 2 == 2 and mesh.shape["mp"] == 2


def solution(mesh):
    in_specs = (
        P("mp", ("groups", "row"), "col"),
        P("mp", ("groups", "row"), "col"),
        P("mp", ("groups", "row"), "col"),
        P("groups"),
    )
    out_specs = (P("mp", ("groups", "row"), "col"), P(("col", "mp"), ("groups", "row")))

    def place(body):
        return jax.shard_map(
            body, mesh=mesh, in_specs=in_specs, out_specs=out_specs, check_vma=False
        )

    def step(queries, keys, values, lengths):
        rollouts = lengths.shape[0] // mesh.shape["groups"]
        kv_local = keys.shape[2] // HEAD_DIM // mesh.shape["col"]
        if not two_hops(mesh, rollouts) or kv_local % 2:
            return place(per_device_general)(queries, keys, values, lengths)
        return place(per_device_paired)(queries, keys, values, lengths)

    return step
```
